16 devices in a mesh: dp: 2 (over y, z), ep: 8 (over x, core).
Axes of the slice: x: 4, y: 2, z: 1, core: 2. Of those that a mesh axis runs over, the one named last changes fastest.
The devices are a block of a 4x4x8 slice.
Arguments:
- x: bfloat16 [2, 8, 384, 2048], P('dp', 'ep'), parts along dimension 0
- expert: int32 [2, 8, 384, 6], P('dp', 'ep'), parts along dimension 0
- slot: int32 [2, 8, 384, 6], P('dp', 'ep'), parts along dimension 0
- gate: float32 [2, 8, 384, 6], P('dp', 'ep'), parts along dimension 0
- w_gate: bfloat16 [64, 2048, 1408], P('ep')
- w_up: bfloat16 [64, 2048, 1408], P('ep')
- w_down: bfloat16 [64, 1408, 2048], P('ep')
- s_gate: bfloat16 [2048, 2816], replicated
- s_up: bfloat16 [2048, 2816], replicated
- s_down: bfloat16 [2816, 2048], replicated
Outputs:
- y: bfloat16 [2, 8, 384, 2048], P('dp', 'ep'), parts along dimension 0
There are 2 independent parts. The reference program is written for one: setup_inputs(seed, part) draws one part's arguments, and reference() takes and returns one part's arrays. A program takes and returns all parts, laid end to end along the dimension named above; an argument that names none is the same for every part.
All inputs are finite; a program needn't handle non-finite values.
Results may differ from the reference program's by a relative error of at most 0.009.
Values are sent between devices in bfloat16 or wider.
A program may use at most 768 MiB of HBM per device.

```python
import jax
import jax.numpy as jnp

MEMBERS = 8
TOKENS = 384
D = 2048
FF = 1408
TOP = 6
EXPERTS = 64
SHARED_FF = 2816
SLOTS = 5 * TOKENS * TOP // (4 * EXPERTS)


def setup_inputs(seed: int = 0, part: int = 0) -> dict:
    own, k1, k2, k3, k4, k5, k6 = jax.random.split(jax.random.key(seed), 7)
    kx, ke, kl, kg = jax.random.split(jax.random.fold_in(own, part), 4)
    devices = (1, MEMBERS)
    place = jax.random.permutation(kl, jnp.arange(EXPERTS, dtype=jnp.uint32))
    slow = ((EXPERTS + (9 * place) % EXPERTS) << ((9 * place) // EXPERTS)) // EXPERTS
    wait = (jax.random.bits(ke, (*devices, TOKENS, EXPERTS), jnp.uint32) >> 10) * slow
    expert = jnp.argsort(wait, axis=-1)[..., :TOP].astype(jnp.int32)
    chosen = jax.nn.one_hot(expert, EXPERTS, dtype=jnp.int32)
    in_line = jnp.cumsum(chosen.reshape(*devices, TOKENS * TOP, EXPERTS), axis=2) - 1
    slot = jnp.sum(in_line.reshape(chosen.shape) * chosen, axis=-1)

    def one(key, rows, columns):
        return (jax.random.normal(key, (rows, columns), jnp.float32) * rows**-0.5).astype(jnp.bfloat16)

    def weights(key, rows, columns):
        return jax.lax.map(lambda k: one(k, rows, columns), jax.random.split(key, EXPERTS))

    return {
        "x": jax.random.normal(kx, (*devices, TOKENS, D), jnp.float32).astype(jnp.bfloat16),
        "expert": expert,
        "slot": slot,
        "gate": jax.nn.softmax(jax.random.normal(kg, expert.shape, jnp.float32)),
        "w_gate": weights(k1, D, FF),
        "w_up": weights(k2, D, FF),
        "w_down": weights(k3, FF, D),
        "s_gate": one(k4, D, SHARED_FF),
        "s_up": one(k5, D, SHARED_FF),
        "s_down": one(k6, SHARED_FF, D),
    }


def einsum(form, a, b):
    return jnp.einsum(form, a.astype(jnp.float32), b.astype(jnp.float32))


def for_all(x, s_gate, s_up, s_down):
    h = jax.nn.silu(einsum("...d,df->...f", x, s_gate)) * einsum("...d,df->...f", x, s_up)
    return einsum("...f,fd->...d", h.astype(jnp.bfloat16), s_down)


def reference(x, expert, slot, gate, w_gate, w_up, w_down, s_gate, s_up, s_down):
    to_expert = jax.nn.one_hot(expert, EXPERTS, dtype=jnp.bfloat16)
    to_slot = jax.nn.one_hot(slot, SLOTS, dtype=jnp.bfloat16)
    weighted = to_expert * gate[..., None].astype(jnp.bfloat16)
    dispatch = einsum("abtke,abtkc->abtec", to_expert, to_slot).astype(jnp.bfloat16)
    combine = einsum("abtke,abtkc->abtec", weighted, to_slot).astype(jnp.bfloat16)
    z = einsum("abtec,abtd->aebcd", dispatch, x).astype(jnp.bfloat16)
    h = jax.nn.silu(einsum("aebcd,edf->aebcf", z, w_gate))
    h = (h * einsum("aebcd,edf->aebcf", z, w_up)).astype(jnp.bfloat16)
    out = einsum("aebcf,efd->aebcd", h, w_down).astype(jnp.bfloat16)
    y = einsum("abtec,aebcd->abtd", combine, out)
    return (y + for_all(x, s_gate, s_up, s_down)).astype(jnp.bfloat16)
```

```python
import jax
import jax.numpy as jnp
from jax import lax
from jax.sharding import PartitionSpec as P

F32, BF16 = jnp.float32, jnp.bfloat16


def dot(form, a, b):
    return jnp.einsum(form, a, b, preferred_element_type=F32)


def solution(mesh):
    def body(x, expert, slot, gate, w_gate, w_up, w_down, s_gate, s_up, s_down):
        x, expert, slot, gate = x[0, 0], expert[0, 0], slot[0, 0], gate[0, 0]
        tokens, top = expert.shape
        mine = w_gate.shape[0]
        slots = 5 * tokens * top // (4 * mine * mesh.shape["ep"])
        place = jnp.where(slot < slots, expert * slots + slot, -1)
        xs = lax.all_gather(x, "ep")
        places = lax.all_gather(place, "ep")
        gates = lax.all_gather(gate, "ep")
        at = places - lax.axis_index("ep") * (mine * slots)
        hot = (at[..., None] == lax.broadcasted_iota(jnp.int32, (1, 1, 1, mine * slots), 3))
        dispatch = jnp.any(hot, axis=2).astype(BF16)
        combine = jnp.sum(jnp.where(hot, gates[..., None], 0), axis=2).astype(BF16)
        z = dot("atr,atd->ard", dispatch, xs).astype(BF16)
        z = z.reshape(z.shape[0], mine, slots, -1).swapaxes(0, 1).reshape(mine, -1, z.shape[-1])
        h = jax.nn.silu(dot("erd,edf->erf", z, w_gate)) * dot("erd,edf->erf", z, w_up)
        out = dot("erf,efd->erd", h.astype(BF16), w_down).astype(BF16)
        out = out.reshape(mine, -1, slots, out.shape[-1]).swapaxes(0, 1).reshape(xs.shape[0], mine * slots, -1)
        y = dot("atr,ard->atd", combine, out).astype(BF16)
        y = lax.psum_scatter(y, "ep")
        hs = jax.nn.silu(dot("td,df->tf", x, s_gate)) * dot("td,df->tf", x, s_up)
        shared = dot("tf,fd->td", hs.astype(BF16), s_down)
        return (y.astype(F32) + shared).astype(BF16)[None, None]

    token, part, whole = P("dp", "ep"), P("ep"), P()
    return jax.shard_map(
        body,
        mesh=mesh,
        in_specs=(token,) * 4 + (part,) * 3 + (whole,) * 3,
        out_specs=token,
        check_vma=False,
    )
```

```python
import functools

import jax
import jax.numpy as jnp
from jax import lax
from jax.experimental import pallas as pl
from jax.experimental.pallas import tpu as pltpu
from jax.sharding import PartitionSpec as P

F32, BF16 = jnp.float32, jnp.bfloat16
MESH = pl.DeviceIdType.MESH
ANY = pl.BlockSpec(memory_space=pl.ANY)
VMEM_LIMIT = 67_043_328

PIECE = 256
OUT = 256
RING = 4
DOWN_RING = 6

OWN, PARTNER, RIGHT, RIGHT_X, FAR, FAR_X, LEFT, LEFT_X = range(8)


def dot(a, b):
    return jnp.dot(a, b, preferred_element_type=F32)


def neighbours(n):
    me = lax.axis_index("ep")
    core = lax.rem(me, 2)
    chip = me // 2

    def at(slot):
        c = core if slot % 2 == 0 else 1 - core
        return 2 * lax.rem(chip + slot // 2, n // 2) + c

    return me, at


def meet(peers):
    barrier = pltpu.get_barrier_semaphore()
    for peer in peers:
        pl.semaphore_signal(barrier, inc=1, device_id={"ep": peer}, device_id_type=MESH)
    pl.semaphore_wait(barrier, len(peers))


def gather_kernel(
    n, slots, x_hbm, info_hbm, wg_hbm, wu_hbm, sg_hbm, su_hbm,
    h_hbm, cw_hbm, hs_hbm,
    xg, info, acc, z, hot, cws, hs, hstage, ring,
    load_sem, info_send, info_recv, send_sem, recv_sem, w_sem, out_sem, cw_sem, h_sem,
):
    me, at = neighbours(n)
    tokens, depth = x_hbm.shape
    experts, _, ff = wg_hbm.shape
    pieces = depth // PIECE
    pad = z.shape[1] // n
    rows = experts * pad
    half = tokens // 2
    shared_steps = 2 * pieces
    total = shared_steps + pieces * experts

    top, bottom, every = pl.ds(0, half), pl.ds(half, half), pl.ds(0, tokens)
    kinds = (
        (OWN, PARTNER, PARTNER, every),
        (OWN, LEFT, RIGHT, every),
        (OWN, RIGHT, LEFT, every),
        (LEFT, FAR, RIGHT, top),
        (RIGHT, FAR, LEFT, bottom),
        (LEFT, LEFT_X, PARTNER, every),
        (RIGHT, RIGHT_X, PARTNER, every),
        (FAR, FAR_X, PARTNER, every),
    )

    def move(kind, k):
        src, dst, to, r = kinds[kind]
        return pltpu.make_async_remote_copy(
            src_ref=xg.at[k, src, r, :],
            dst_ref=xg.at[k, dst, r, :],
            send_sem=send_sem.at[kind, k],
            recv_sem=recv_sem.at[kind, k],
            device_id={"ep": at(to)},
            device_id_type=MESH,
        )

    def opposite(slot):
        return 2 * ((n // 2 - slot // 2) % (n // 2)) + slot % 2

    def tell(slot):
        back = opposite(slot)
        return pltpu.make_async_remote_copy(
            src_ref=info.at[OWN],
            dst_ref=info.at[back],
            send_sem=info_send.at[slot],
            recv_sem=info_recv.at[back],
            device_id={"ep": at(slot)},
            device_id_type=MESH,
        )

    def load_x(k):
        return pltpu.make_async_copy(x_hbm.at[:, pl.ds(k * PIECE, PIECE)], xg.at[k, OWN], load_sem.at[k])

    load_info = pltpu.make_async_copy(info_hbm, info.at[OWN], load_sem.at[pieces])

    def fetch_shared(which, k, slot):
        w = (sg_hbm, su_hbm)[which]
        return pltpu.make_async_copy(w.at[pl.ds(k * PIECE, PIECE), :], ring.at[slot], w_sem.at[slot, 0])

    def fetch_routed(k, e, slot):
        return (
            pltpu.make_async_copy(wg_hbm.at[e, pl.ds(k * PIECE, PIECE), :], ring.at[slot, :, pl.ds(0, ff)], w_sem.at[slot, 0]),
            pltpu.make_async_copy(wu_hbm.at[e, pl.ds(k * PIECE, PIECE), :], ring.at[slot, :, pl.ds(ff, ff)], w_sem.at[slot, 1]),
        )

    def start(i):
        slot = lax.rem(i, RING)

        @pl.when(i < pieces)
        def _():
            fetch_shared(0, i, slot).start()

        @pl.when((i >= pieces) & (i < shared_steps))
        def _():
            fetch_shared(1, i - pieces, slot).start()

        @pl.when((i >= shared_steps) & (i < total))
        def _():
            j = i - shared_steps
            for c in fetch_routed(j // experts, lax.rem(j, experts), slot):
                c.start()

    def accumulate(a, left, slot, first):
        width = ring.shape[2]
        for lo in range(0, width, 256):
            cut = pl.ds(lo, min(256, width - lo))
            before = jnp.where(first, 0.0, acc[a, :, cut])
            acc[a, :, cut] = before + dot(left, ring[slot, :, cut])

    for k in range(pieces):
        load_x(k).start()
    load_info.start()
    for i in range(RING - 1):
        fetch_shared(0, i, i).start()
    meet([at(s) for s in range(1, n)])
    for k in range(pieces):
        load_x(k).wait()
        if k < 2:
            move(1, k).start()
            move(2, k).start()
        move(0, k).start()
        if k == 0:
            load_info.wait()
            for s in range(1, n):
                tell(s).start()

    def shared_step(i, _):
        slot = lax.rem(i, RING)
        start(i + RING - 1)
        fetch_shared(0, 0, slot).wait()
        k = lax.rem(i, pieces)
        accumulate(i // pieces, xg[k, OWN], slot, k == 0)
        return 0

    lax.fori_loop(0, shared_steps, shared_step, 0)

    def near(k):
        move(1, k).wait_recv()
        move(2, k).wait_recv()
        move(3, k).start()
        move(4, k).start()
        move(5, k).start()
        move(6, k).start()

        @pl.when(k + 2 < pieces)
        def _():
            move(1, k + 2).start()
            move(2, k + 2).start()

    near(0)

    width = ring.shape[2]
    for lo in range(0, width, 256):
        cut = pl.ds(lo, min(256, width - lo))
        hs[:, cut] = (jax.nn.silu(acc[0, :, cut]) * acc[1, :, cut]).astype(BF16)
    hs_out = pltpu.make_async_copy(hs, hs_hbm, out_sem)
    hs_out.start()

    base = (me * rows).astype(F32)
    row = lax.broadcasted_iota(jnp.int32, (rows, tokens), 0).astype(F32) + base
    top_k = info.shape[1] // 2

    for s in range(n):
        if s:
            tell(opposite(s)).wait_recv()
        found = jnp.zeros((rows, tokens), F32)
        for j in range(top_k):
            found = jnp.where(row == info[s, pl.ds(j, 1), :], 1.0, found)
        hot[s] = found.astype(BF16)

    def weigh(s):
        found = jnp.zeros((rows, tokens), F32)
        for j in range(top_k):
            found = jnp.where(row == info[s, pl.ds(j, 1), :], info[s, pl.ds(top_k + j, 1), :], found)
        return found.T.astype(BF16)

    def cw_out(s):
        return pltpu.make_async_copy(cws.at[lax.rem(s, 2)], cw_hbm.at[s], cw_sem.at[lax.rem(s, 2)])

    def dispatch(k):
        move(0, k).wait_recv()
        move(5, k).wait_recv()
        move(6, k).wait_recv()

        def place(s):
            got = dot(hot[s], xg[k, s]).astype(BF16)
            for e in range(experts):
                z[e, s * pad : (s + 1) * pad, :] = got[e * pad : (e + 1) * pad]

        for s in (OWN, PARTNER, RIGHT, LEFT, RIGHT_X, LEFT_X):
            place(s)
        move(3, k).wait_recv()
        move(4, k).wait_recv()
        move(7, k).start()
        place(FAR)
        move(7, k).wait_recv()
        place(FAR_X)

    def piece(k, _):
        dispatch(k)

        def step(e, _):
            i = shared_steps + k * experts + e
            slot = lax.rem(i, RING)
            start(i + RING - 1)
            for c in fetch_routed(0, 0, slot):
                c.wait()
            accumulate(e, z[e], slot, k == 0)

            @pl.when(e == experts // 2 - 1)
            def _():
                near(k + 1)

            return 0

        lax.fori_loop(0, experts, step, 0)

        @pl.when(k >= 2)
        def _():
            cw_out(k - 2).wait()

        cws[lax.rem(k, 2)] = weigh(k)
        cw_out(k).start()
        return 0

    assert pieces == n
    lax.fori_loop(0, pieces - 1, piece, 0)
    last = pieces - 1
    dispatch(last)

    def h_out(e):
        return pltpu.make_async_copy(hstage.at[lax.rem(e, 2)], h_hbm.at[e], h_sem.at[lax.rem(e, 2)])

    def final_step(e, _):
        i = shared_steps + last * experts + e
        slot = lax.rem(i, RING)
        start(i + RING - 1)
        for c in fetch_routed(0, 0, slot):
            c.wait()

        @pl.when(e >= 2)
        def _():
            h_out(e - 2).wait()

        for lo in range(0, ff, 256):
            size = min(256, ff - lo)
            a, b = pl.ds(lo, size), pl.ds(ff + lo, size)
            g = acc[e, :, a] + dot(z[e], ring[slot, :, a])
            u = acc[e, :, b] + dot(z[e], ring[slot, :, b])
            hstage[lax.rem(e, 2), :, a] = (jax.nn.silu(g) * u).astype(BF16)
        h_out(e).start()
        return 0

    lax.fori_loop(0, experts, final_step, 0)
    cw_out(last - 2).wait()
    cws[last % 2] = weigh(last)
    cw_out(last).start()

    for s in (last - 1, last):
        cw_out(s).wait()
    for e in (experts - 2, experts - 1):
        h_out(e).wait()
    hs_out.wait()
    for s in range(1, n):
        tell(s).wait_send()

    def drain(k, _):
        for kind in range(len(kinds)):
            move(kind, k).wait_send()
        return 0

    lax.fori_loop(0, pieces, drain, 0)


def reduce_kernel(
    n, h_hbm, cw_hbm, hs_hbm, wd_hbm, sd_hbm,
    y_hbm,
    h, cw, hs, out, ynear, yown, pair_out, far_out, near_out, ystage, pair_in, far_in, near_in, ring, sring,
    load_sem, pair_send, pair_recv, far_send, far_recv, near_send, near_recv, w_sem, s_sem, y_sem,
):
    me, at = neighbours(n)
    experts, rows_e, ff = h_hbm.shape
    tokens, depth = y_hbm.shape
    chunks = depth // OUT
    pad = rows_e // n
    half = tokens // 2
    total = chunks * experts

    def columns(c):
        return pl.ds(pl.multiple_of(c * OUT, OUT), OUT)

    def load_h(e):
        return pltpu.make_async_copy(h_hbm.at[e], h.at[e], load_sem.at[e])

    load_cw = pltpu.make_async_copy(cw_hbm, cw, load_sem.at[experts])
    load_hs = pltpu.make_async_copy(hs_hbm, hs, load_sem.at[experts + 1])

    def fetch(i):
        slot = lax.rem(i, DOWN_RING)
        return pltpu.make_async_copy(
            wd_hbm.at[lax.rem(i, experts), :, columns(i // experts)], ring.at[slot], w_sem.at[slot]
        )

    def fetch_shared(c):
        slot = lax.rem(c, 2)
        return pltpu.make_async_copy(sd_hbm.at[:, columns(c)], sring.at[slot], s_sem.at[slot])

    other = (FAR_X, RIGHT_X, LEFT_X, PARTNER)
    I_FAR, I_RIGHT, I_LEFT, I_OWN = range(4)

    def pair(i, c):
        return pltpu.make_async_remote_copy(
            src_ref=pair_out.at[lax.rem(c, 2), i],
            dst_ref=pair_in.at[c, i],
            send_sem=pair_send.at[i, lax.rem(c, 2)],
            recv_sem=pair_recv.at[i, c],
            device_id={"ep": at(PARTNER)},
            device_id_type=MESH,
        )

    def far(side, c):
        return pltpu.make_async_remote_copy(
            src_ref=far_out.at[lax.rem(c, 2), pl.ds(side * half, half), :],
            dst_ref=far_in.at[c, side],
            send_sem=far_send.at[side, lax.rem(c, 2)],
            recv_sem=far_recv.at[side, c],
            device_id={"ep": at((RIGHT, LEFT)[side])},
            device_id_type=MESH,
        )

    def near(side, c):
        return pltpu.make_async_remote_copy(
            src_ref=near_out.at[lax.rem(c, 2), side],
            dst_ref=near_in.at[c, side],
            send_sem=near_send.at[side, lax.rem(c, 2)],
            recv_sem=near_recv.at[side, c],
            device_id={"ep": at((RIGHT, LEFT)[side])},
            device_id_type=MESH,
        )

    def result(c):
        slot = lax.rem(c, 2)
        return pltpu.make_async_copy(ystage.at[slot], y_hbm.at[:, columns(c)], y_sem.at[slot])

    load_h(0).start()
    for i in range(DOWN_RING - 1):
        fetch(i).start()
        if i + 1 < experts:
            load_h(i + 1).start()
    for e in range(DOWN_RING, experts):
        load_h(e).start()
    load_cw.start()
    load_hs.start()
    fetch_shared(0).start()
    meet([at(s) for s in (PARTNER, RIGHT, LEFT)])

    def make(c):
        def step(e, _):
            i = c * experts + e

            @pl.when(i + DOWN_RING - 1 < total)
            def _():
                fetch(i + DOWN_RING - 1).start()

            fetch(i).wait()

            @pl.when(c == 0)
            def _():
                load_h(e).wait()

            got = dot(h[e], ring[lax.rem(i, DOWN_RING)]).astype(BF16)
            at_row = pl.ds(pl.multiple_of(e * pad, pad), pad)
            for s in range(n):
                out[s, at_row, :] = got[s * pad : (s + 1) * pad]
            return 0

        lax.fori_loop(0, experts, step, 0)

        @pl.when(c == 0)
        def _():
            load_cw.wait()
            load_hs.wait()

        @pl.when(c >= 2)
        def _():
            for i in range(4):
                pair(i, c - 2).wait_send()
            for side in range(2):
                far(side, c - 2).wait_send()

        @pl.when(c + 1 < chunks)
        def _():
            fetch_shared(c + 1).start()

        for i in range(4):
            s = other[i]
            pair_out[lax.rem(c, 2), i] = dot(cw[s], out[s]).astype(BF16)
            pair(i, c).start()
        ynear[lax.rem(c, 2), 0] = dot(cw[RIGHT], out[RIGHT])
        ynear[lax.rem(c, 2), 1] = dot(cw[LEFT], out[LEFT])
        fetch_shared(c).wait()
        yown[lax.rem(c, 4)] = dot(hs[...], sring[lax.rem(c, 2)]) + dot(cw[OWN], out[OWN])
        mine = dot(cw[FAR], out[FAR])
        pair(I_FAR, c).wait_recv()
        far_out[lax.rem(c, 2)] = (mine + pair_in[c, I_FAR].astype(F32)).astype(BF16)
        far(0, c).start()
        far(1, c).start()

    def pass_on(c):
        slot = lax.rem(c, 2)

        @pl.when(c >= 2)
        def _():
            for side in range(2):
                near(side, c - 2).wait_send()

        for side, i in ((0, I_RIGHT), (1, I_LEFT)):
            pair(i, c).wait_recv()
            far(side, c).wait_recv()
            both, alone = pl.ds(side * half, half), pl.ds((1 - side) * half, half)
            near_out[slot, side, alone] = (ynear[slot, side, alone] + pair_in[c, i, alone].astype(F32)).astype(BF16)
            near_out[slot, side, both] = (
                ynear[slot, side, both] + pair_in[c, i, both].astype(F32) + far_in[c, side].astype(F32)
            ).astype(BF16)
            near(side, c).start()

    def finish(c):
        slot = lax.rem(c, 2)

        @pl.when(c >= 2)
        def _():
            result(c - 2).wait()

        pair(I_OWN, c).wait_recv()
        near(0, c).wait_recv()
        near(1, c).wait_recv()
        ystage[slot] = (
            yown[lax.rem(c, 4)]
            + pair_in[c, I_OWN].astype(F32)
            + near_in[c, 0].astype(F32)
            + near_in[c, 1].astype(F32)
        ).astype(BF16)
        result(c).start()

    def chunk(c, _):
        @pl.when(c < chunks)
        def _():
            make(c)

        @pl.when((c >= 1) & (c <= chunks))
        def _():
            pass_on(c - 1)

        @pl.when(c >= 3)
        def _():
            finish(c - 3)

        return 0

    lax.fori_loop(0, chunks + 3, chunk, 0)
    for c in (chunks - 2, chunks - 1):
        result(c).wait()
        for i in range(4):
            pair(i, c).wait_send()
        for side in range(2):
            far(side, c).wait_send()
            near(side, c).wait_send()


def solution(mesh):
    n = mesh.shape["ep"]
    assert n == 8

    def body(x, expert, slot, gate, w_gate, w_up, w_down, s_gate, s_up, s_down):
        x, expert, slot, gate = x[0, 0], expert[0, 0], slot[0, 0], gate[0, 0]
        (tokens, depth), top = x.shape, expert.shape[1]
        experts, _, ff = w_gate.shape
        shared = s_gate.shape[1]
        slots = 5 * tokens * top // (4 * experts * n)
        pad = -(-slots // 16) * 16
        rows = experts * pad
        pieces, chunks, half = depth // PIECE, depth // OUT, tokens // 2
        top_k = 8
        assert top <= top_k and shared == 2 * ff and rows % 128 == 0
        place = jnp.where(slot < slots, expert * pad + slot, -1).astype(F32)
        grow = ((0, 0), (0, top_k - top))
        info = jnp.concatenate([jnp.pad(place, grow, constant_values=-1), jnp.pad(gate, grow)], axis=1).T

        dma = pltpu.SemaphoreType.DMA
        h, cw, hs = pl.pallas_call(
            functools.partial(gather_kernel, n, slots),
            out_shape=(
                jax.ShapeDtypeStruct((experts, n * pad, ff), BF16),
                jax.ShapeDtypeStruct((n, tokens, rows), BF16),
                jax.ShapeDtypeStruct((tokens, shared), BF16),
            ),
            in_specs=[ANY] * 6,
            out_specs=(ANY,) * 3,
            scratch_shapes=[
                pltpu.VMEM((pieces, n, tokens, PIECE), BF16),
                pltpu.VMEM((n, 2 * top_k, tokens), F32),
                pltpu.VMEM((experts, n * pad, 2 * ff), F32),
                pltpu.VMEM((experts, n * pad, PIECE), BF16),
                pltpu.VMEM((n, rows, tokens), BF16),
                pltpu.VMEM((2, tokens, rows), BF16),
                pltpu.VMEM((tokens, shared), BF16),
                pltpu.VMEM((2, n * pad, ff), BF16),
                pltpu.VMEM((RING, PIECE, 2 * ff), BF16),
                dma((pieces + 1,)),
                dma((n,)),
                dma((n,)),
                dma((8, pieces)),
                dma((8, pieces)),
                dma((RING, 2)),
                dma,
                dma((2,)),
                dma((2,)),
            ],
            compiler_params=pltpu.CompilerParams(
                collective_id=0, has_side_effects=True, vmem_limit_bytes=VMEM_LIMIT
            ),
            name="gather",
        )(x, info, w_gate, w_up, s_gate, s_up)
        y = pl.pallas_call(
            functools.partial(reduce_kernel, n),
            out_shape=jax.ShapeDtypeStruct((tokens, depth), BF16),
            in_specs=[ANY] * 5,
            out_specs=ANY,
            scratch_shapes=[
                pltpu.VMEM((experts, n * pad, ff), BF16),
                pltpu.VMEM((n, tokens, rows), BF16),
                pltpu.VMEM((tokens, shared), BF16),
                pltpu.VMEM((n, rows, OUT), BF16),
                pltpu.VMEM((2, 2, tokens, OUT), F32),
                pltpu.VMEM((4, tokens, OUT), F32),
                pltpu.VMEM((2, 4, tokens, OUT), BF16),
                pltpu.VMEM((2, tokens, OUT), BF16),
                pltpu.VMEM((2, 2, tokens, OUT), BF16),
                pltpu.VMEM((2, tokens, OUT), BF16),
                pltpu.VMEM((chunks, 4, tokens, OUT), BF16),
                pltpu.VMEM((chunks, 2, half, OUT), BF16),
                pltpu.VMEM((chunks, 2, tokens, OUT), BF16),
                pltpu.VMEM((DOWN_RING, ff, OUT), BF16),
                pltpu.VMEM((2, shared, OUT), BF16),
                dma((experts + 2,)),
                dma((4, 2)),
                dma((4, chunks)),
                dma((2, 2)),
                dma((2, chunks)),
                dma((2, 2)),
                dma((2, chunks)),
                dma((DOWN_RING,)),
                dma((2,)),
                dma((2,)),
            ],
            compiler_params=pltpu.CompilerParams(
                collective_id=1, has_side_effects=True, vmem_limit_bytes=VMEM_LIMIT
            ),
            name="reduce",
        )(h, cw, hs, w_down, s_down)
        return y[None, None]

    token, part, whole = P("dp", "ep"), P("ep"), P()
    return jax.shard_map(
        body,
        mesh=mesh,
        in_specs=(token,) * 4 + (part,) * 3 + (whole,) * 3,
        out_specs=token,
        check_vma=False,
    )
```

```python
import functools

import jax
import jax.numpy as jnp
from jax import lax
from jax.experimental import pallas as pl
from jax.experimental.pallas import tpu as pltpu
from jax.sharding import PartitionSpec as P

F32, BF16 = jnp.float32, jnp.bfloat16
MESH = pl.DeviceIdType.MESH
ANY = pl.BlockSpec(memory_space=pl.ANY)
VMEM_LIMIT = 67_043_328

PIECE = 256
UNIT = 512
OUT = 256
AHEAD = 2
RING = 3
SPLIT = 5
SLAB = 512
DOWN_RING = 8

OWN, PARTNER, RIGHT, RIGHT_X, FAR, FAR_X, LEFT, LEFT_X = range(8)


def dot(a, b):
    return jnp.dot(a, b, preferred_element_type=F32)


def neighbours(n):
    me = lax.axis_index("ep")
    core = lax.rem(me, 2)
    chip = me // 2

    def at(slot):
        c = core if slot % 2 == 0 else 1 - core
        return 2 * lax.rem(chip + slot // 2, n // 2) + c

    return me, at


def meet(peers):
    barrier = pltpu.get_barrier_semaphore()
    for peer in peers:
        pl.semaphore_signal(barrier, inc=1, device_id={"ep": peer}, device_id_type=MESH)
    pl.semaphore_wait(barrier, len(peers))


def gather_kernel(
    n, slots, x_hbm, info_hbm, wg_hbm, wu_hbm, sg_hbm, su_hbm,
    h_hbm, cw_hbm, hs_hbm,
    xg, info, acc, z, hot, cws, hstage, ring,
    load_sem, info_send, info_recv, send_sem, recv_sem, w_sem, cw_sem, h_sem,
):
    me, at = neighbours(n)
    tokens, depth = x_hbm.shape
    experts, _, ff = wg_hbm.shape
    pieces = depth // PIECE
    pad = z.shape[1] // n
    rows = experts * pad
    half = tokens // 2
    units, per = depth // UNIT, UNIT // PIECE
    shared_steps = 2 * units
    total = shared_steps + units * experts

    top, bottom, every = pl.ds(0, half), pl.ds(half, half), pl.ds(0, tokens)
    kinds = (
        (OWN, PARTNER, PARTNER, every),
        (OWN, LEFT, RIGHT, every),
        (OWN, RIGHT, LEFT, every),
        (LEFT, FAR, RIGHT, top),
        (RIGHT, FAR, LEFT, bottom),
        (LEFT, LEFT_X, PARTNER, every),
        (RIGHT, RIGHT_X, PARTNER, every),
        (FAR, FAR_X, PARTNER, every),
    )

    def move(kind, k):
        src, dst, to, r = kinds[kind]
        return pltpu.make_async_remote_copy(
            src_ref=xg.at[k, src, r, :],
            dst_ref=xg.at[k, dst, r, :],
            send_sem=send_sem.at[kind, k],
            recv_sem=recv_sem.at[kind, k],
            device_id={"ep": at(to)},
            device_id_type=MESH,
        )

    def opposite(slot):
        return 2 * ((n // 2 - slot // 2) % (n // 2)) + slot % 2

    def tell(slot):
        back = opposite(slot)
        return pltpu.make_async_remote_copy(
            src_ref=info.at[OWN],
            dst_ref=info.at[back],
            send_sem=info_send.at[slot],
            recv_sem=info_recv.at[back],
            device_id={"ep": at(slot)},
            device_id_type=MESH,
        )

    def load_x(k):
        return pltpu.make_async_copy(x_hbm.at[:, pl.ds(k * PIECE, PIECE)], xg.at[k, OWN], load_sem.at[k])

    load_info = pltpu.make_async_copy(info_hbm, info.at[OWN], load_sem.at[pieces])

    def fetch_shared(which, k, slot):
        w = (sg_hbm, su_hbm)[which]
        return pltpu.make_async_copy(w.at[pl.ds(k * UNIT, UNIT), :], ring.at[slot], w_sem.at[slot, 0])

    def fetch_routed(k, e, slot):
        return (
            pltpu.make_async_copy(wg_hbm.at[e, pl.ds(k * UNIT, UNIT), :], ring.at[slot, :, pl.ds(0, ff)], w_sem.at[slot, 0]),
            pltpu.make_async_copy(wu_hbm.at[e, pl.ds(k * UNIT, UNIT), :], ring.at[slot, :, pl.ds(ff, ff)], w_sem.at[slot, 1]),
        )

    def start(i):
        slot = lax.rem(i, RING)

        @pl.when(i < units)
        def _():
            fetch_shared(0, i, slot).start()

        @pl.when((i >= units) & (i < shared_steps))
        def _():
            fetch_shared(1, i - units, slot).start()

        @pl.when((i >= shared_steps) & (i < total))
        def _():
            j = i - shared_steps
            for c in fetch_routed(j // experts, lax.rem(j, experts), slot):
                c.start()

    def accumulate(a, left, slot, first):
        width = ring.shape[2]
        for lo in range(0, width, 256):
            cut = pl.ds(lo, min(256, width - lo))
            before = jnp.where(first, 0.0, acc[a, :, cut])
            acc[a, :, cut] = before + dot(left, ring[slot, :, cut])

    for k in range(pieces):
        load_x(k).start()
    load_info.start()
    for i in range(RING - 1):
        fetch_shared(0, i, i).start()
    meet([at(s) for s in range(1, n)])
    for k in range(pieces):
        load_x(k).wait()
        if k < AHEAD:
            move(1, k).start()
            move(2, k).start()
        move(0, k).start()
        if k == 0:
            load_info.wait()
            for s in range(1, n):
                tell(s).start()

    def near(k):
        move(1, k).wait_recv()
        move(2, k).wait_recv()
        move(3, k).start()
        move(4, k).start()
        move(5, k).start()
        move(6, k).start()

        @pl.when(k + AHEAD < pieces)
        def _():
            move(1, k + AHEAD).start()
            move(2, k + AHEAD).start()

    def far(k):
        move(3, k).wait_recv()
        move(4, k).wait_recv()
        move(7, k).start()

    def shared_step(i, _):
        slot = lax.rem(i, RING)
        start(i + RING - 1)
        fetch_shared(0, 0, slot).wait()
        u = lax.rem(i, units)
        mine = jnp.concatenate([xg[u * per + p, OWN] for p in range(per)], axis=1)
        accumulate(i // units, mine, slot, u == 0)

        @pl.when(i == shared_steps - 3)
        def _():
            near(0)

        return 0

    lax.fori_loop(0, shared_steps, shared_step, 0)

    def hs_out(i):
        return pltpu.make_async_copy(hstage.at[i], hs_hbm.at[i], h_sem.at[i])

    for i in range(2):
        for lo in range(0, ff, 256):
            size = min(256, ff - lo)
            cut = pl.ds(i * ff + lo, size)
            hstage[i, :, pl.ds(lo, size)] = (jax.nn.silu(acc[0, :, cut]) * acc[1, :, cut]).astype(BF16)
        hs_out(i).start()

    top_k = info.shape[1] // 2
    first_row = (me * experts + lax.broadcasted_iota(jnp.int32, (experts, tokens), 0)) * pad
    first_row = first_row.astype(F32)
    in_slot = lax.broadcasted_iota(jnp.int32, (pad, tokens), 0).astype(F32)

    def table(s, weighted):
        at_slot = jnp.full((experts, tokens), -1.0, F32)
        weight = jnp.zeros((experts, tokens), F32)
        for j in range(top_k):
            here = info[s, pl.ds(j, 1), :] - first_row
            hit = (here >= 0) & (here < pad)
            at_slot = jnp.where(hit, here, at_slot)
            if weighted:
                weight = jnp.where(hit, info[s, pl.ds(top_k + j, 1), :], weight)
        return at_slot, weight

    for s in range(n):
        if s:
            tell(opposite(s)).wait_recv()
        at_slot, _ = table(s, False)
        for e in range(experts):
            hit = in_slot == at_slot[e : e + 1]
            hot[s, pl.ds(e * pad, pad), :] = jnp.where(hit, 1.0, 0.0).astype(BF16)

    near(1)

    def weigh(s):
        at_slot, weight = table(s, True)
        found = [jnp.where(in_slot == at_slot[e : e + 1], weight[e : e + 1], 0.0) for e in range(experts)]
        return jnp.concatenate(found, axis=0).T.astype(BF16)

    def cw_out(s):
        return pltpu.make_async_copy(cws.at[lax.rem(s, 2)], cw_hbm.at[s], cw_sem.at[lax.rem(s, 2)])

    def place(k, p, sources):
        for s in sources:
            got = dot(hot[s], xg[k, s]).astype(BF16)
            for e in range(experts):
                z[e, s * pad : (s + 1) * pad, pl.ds(p * PIECE, PIECE)] = got[e * pad : (e + 1) * pad]

    def place_near(k, p):
        move(0, k).wait_recv()
        move(5, k).wait_recv()
        move(6, k).wait_recv()
        place(k, p, (OWN, PARTNER, RIGHT, LEFT, RIGHT_X, LEFT_X))

    def place_far(k, p):
        place(k, p, (FAR,))
        move(7, k).wait_recv()
        place(k, p, (FAR_X,))

    def weigh_out(s):
        @pl.when(s >= 2)
        def _():
            cw_out(s - 2).wait()

        cws[lax.rem(s, 2)] = weigh(s)
        cw_out(s).start()

    assert per == 2

    def weigh_all(s, _):
        weigh_out(s)
        return 0

    lax.fori_loop(0, n, weigh_all, 0)
    far(0)
    place_near(0, 0)
    place_near(1, 1)
    near(2)
    far(1)
    place_far(0, 0)
    place_far(1, 1)

    def unit(u, _):
        def step(e, _):
            i = shared_steps + u * experts + e
            slot = lax.rem(i, RING)
            start(i + RING - 1)
            for c in fetch_routed(0, 0, slot):
                c.wait()
            accumulate(e, z[e], slot, u == 0)

            @pl.when((e == 1) | ((e == 6) & (2 * u + 4 < pieces)))
            def _():
                near(2 * u + 3 + e // 6)

            @pl.when(e == 4)
            def _():
                far(2 * u + 2)

            return 0

        lax.fori_loop(0, experts, step, 0)
        k = 2 * u + 2
        place_near(k, 0)
        place_far(k, 0)
        far(k + 1)
        place_near(k + 1, 1)
        place_far(k + 1, 1)
        return 0

    lax.fori_loop(0, units - 1, unit, 0)
    for i in range(2):
        hs_out(i).wait()
    last = units - 1

    def h_out(e):
        return pltpu.make_async_copy(hstage.at[lax.rem(e, 2)], h_hbm.at[e], h_sem.at[lax.rem(e, 2)])

    def final_step(e, _):
        i = shared_steps + last * experts + e
        slot = lax.rem(i, RING)
        start(i + RING - 1)
        for c in fetch_routed(0, 0, slot):
            c.wait()

        @pl.when(e >= 2)
        def _():
            h_out(e - 2).wait()

        for lo in range(0, ff, 256):
            size = min(256, ff - lo)
            a, b = pl.ds(lo, size), pl.ds(ff + lo, size)
            g = acc[e, :, a] + dot(z[e], ring[slot, :, a])
            u = acc[e, :, b] + dot(z[e], ring[slot, :, b])
            hstage[lax.rem(e, 2), :, a] = (jax.nn.silu(g) * u).astype(BF16)
        h_out(e).start()
        return 0

    lax.fori_loop(0, experts, final_step, 0)

    for s in (n - 2, n - 1):
        cw_out(s).wait()
    for e in (experts - 2, experts - 1):
        h_out(e).wait()
    for s in range(1, n):
        tell(s).wait_send()

    def drain(k, _):
        for kind in range(len(kinds)):
            move(kind, k).wait_send()
        return 0

    lax.fori_loop(0, pieces, drain, 0)


def reduce_kernel(
    n, h_hbm, cw_hbm, hs_hbm, wd_hbm, sd_hbm,
    y_hbm,
    h, cw, hs, out, yshared, ynear, yown, pair_out, far_out, near_out, ystage, pair_in, far_in, near_in, ring, sring,
    load_sem, pair_send, pair_recv, far_send, far_recv, near_send, near_recv, w_sem, s_sem, y_sem,
):
    me, at = neighbours(n)
    experts, rows_e, ff = h_hbm.shape
    tokens, depth = y_hbm.shape
    chunks = depth // OUT
    pad = rows_e // n
    half = tokens // 2
    per = SLAB // OUT
    slabs = chunks // per
    total = slabs * experts

    def columns(c):
        return pl.ds(pl.multiple_of(c * OUT, OUT), OUT)

    def load_h(e):
        return pltpu.make_async_copy(h_hbm.at[e], h.at[e], load_sem.at[e])

    load_cw = pltpu.make_async_copy(cw_hbm, cw, load_sem.at[experts])
    load_hs = pltpu.make_async_copy(hs_hbm, hs, load_sem.at[experts + 1])

    def slab(q):
        return pl.ds(pl.multiple_of(q * SLAB, SLAB), SLAB)

    def fetch(i):
        slot = lax.rem(i, DOWN_RING)
        return pltpu.make_async_copy(
            wd_hbm.at[lax.rem(i, experts), :, slab(i // experts)], ring.at[slot], w_sem.at[slot]
        )

    def fetch_shared(q):
        slot = lax.rem(q, 2)
        return pltpu.make_async_copy(sd_hbm.at[:, slab(q)], sring.at[slot], s_sem.at[slot])

    other = (FAR_X, RIGHT_X, LEFT_X, PARTNER)
    I_FAR, I_RIGHT, I_LEFT, I_OWN = range(4)

    def pair(i, c):
        return pltpu.make_async_remote_copy(
            src_ref=pair_out.at[lax.rem(c, 2), i],
            dst_ref=pair_in.at[c, i],
            send_sem=pair_send.at[i, lax.rem(c, 2)],
            recv_sem=pair_recv.at[i, c],
            device_id={"ep": at(PARTNER)},
            device_id_type=MESH,
        )

    def far(side, c):
        return pltpu.make_async_remote_copy(
            src_ref=far_out.at[lax.rem(c, 2), pl.ds(side * half, half), :],
            dst_ref=far_in.at[c, side],
            send_sem=far_send.at[side, lax.rem(c, 2)],
            recv_sem=far_recv.at[side, c],
            device_id={"ep": at((RIGHT, LEFT)[side])},
            device_id_type=MESH,
        )

    def near(side, c):
        return pltpu.make_async_remote_copy(
            src_ref=near_out.at[lax.rem(c, 2), side],
            dst_ref=near_in.at[c, side],
            send_sem=near_send.at[side, lax.rem(c, 2)],
            recv_sem=near_recv.at[side, c],
            device_id={"ep": at((RIGHT, LEFT)[side])},
            device_id_type=MESH,
        )

    def result(c):
        slot = lax.rem(c, 2)
        return pltpu.make_async_copy(ystage.at[slot], y_hbm.at[:, columns(c)], y_sem.at[slot])

    load_h(0).start()
    for i in range(experts):
        fetch(i).start()
        if i + 1 < experts:
            load_h(i + 1).start()
    load_cw.start()
    load_hs.start()
    fetch_shared(0).start()
    for i in range(experts, DOWN_RING):
        fetch(i).start()
    fetch_shared(1).start()
    meet([at(s) for s in (PARTNER, RIGHT, LEFT)])

    def down(q, begin, end, first=False):
        side = lax.rem(q, 2)

        def step(e, _):
            i = q * experts + e
            slot = lax.rem(i, DOWN_RING)
            fetch(i).wait()
            if first:
                load_h(e).wait()
            got = dot(h[e], ring[slot]).astype(BF16)
            at_row = pl.ds(pl.multiple_of(e * pad, pad), pad)
            for p in range(per):
                for s in range(n):
                    out[side, p, s, at_row, :] = got[s * pad : (s + 1) * pad, p * OUT : (p + 1) * OUT]

            @pl.when(i + DOWN_RING < total)
            def _():
                fetch(i + DOWN_RING).start()

            return 0

        lax.fori_loop(begin, min(end, experts), step, 0)
        if end > experts:
            fetch_shared(q).wait()
            if first:
                load_hs.wait()
            got = dot(jnp.concatenate([hs[0], hs[1]], axis=1), sring[side])
            for p in range(per):
                yshared[side, p] = got[:, p * OUT : (p + 1) * OUT]

            @pl.when(q + 2 < slabs)
            def _():
                fetch_shared(q + 2).start()

    def make(c):
        side, p = lax.rem(c // per, 2), lax.rem(c, per)

        @pl.when(c >= 2)
        def _():
            for i in range(4):
                pair(i, c - 2).wait_send()
            for way in range(2):
                far(way, c - 2).wait_send()

        for i in range(4):
            s = other[i]
            pair_out[lax.rem(c, 2), i] = dot(cw[s], out[side, p, s]).astype(BF16)
            pair(i, c).start()
        ynear[lax.rem(c, 2), 0] = dot(cw[RIGHT], out[side, p, RIGHT])
        ynear[lax.rem(c, 2), 1] = dot(cw[LEFT], out[side, p, LEFT])
        yown[lax.rem(c, 4)] = yshared[side, p] + dot(cw[OWN], out[side, p, OWN])
        mine = dot(cw[FAR], out[side, p, FAR])
        pair(I_FAR, c).wait_recv()
        far_out[lax.rem(c, 2)] = (mine + pair_in[c, I_FAR].astype(F32)).astype(BF16)
        far(0, c).start()
        far(1, c).start()
        for j in range(per):

            @pl.when((p == j) & (c // per + 1 < slabs))
            def _():
                down(c // per + 1, (0, SPLIT)[j], (SPLIT, experts + 1)[j])

    def pass_on(c):
        slot = lax.rem(c, 2)

        @pl.when(c >= 2)
        def _():
            for side in range(2):
                near(side, c - 2).wait_send()

        for side, i in ((0, I_RIGHT), (1, I_LEFT)):
            pair(i, c).wait_recv()
            far(side, c).wait_recv()
            both, alone = pl.ds(side * half, half), pl.ds((1 - side) * half, half)
            near_out[slot, side, alone] = (ynear[slot, side, alone] + pair_in[c, i, alone].astype(F32)).astype(BF16)
            near_out[slot, side, both] = (
                ynear[slot, side, both] + pair_in[c, i, both].astype(F32) + far_in[c, side].astype(F32)
            ).astype(BF16)
            near(side, c).start()

    def finish(c):
        slot = lax.rem(c, 2)

        @pl.when(c >= 2)
        def _():
            result(c - 2).wait()

        pair(I_OWN, c).wait_recv()
        near(0, c).wait_recv()
        near(1, c).wait_recv()
        ystage[slot] = (
            yown[lax.rem(c, 4)]
            + pair_in[c, I_OWN].astype(F32)
            + near_in[c, 0].astype(F32)
            + near_in[c, 1].astype(F32)
        ).astype(BF16)
        result(c).start()

    def chunk(c, _):
        @pl.when(c < chunks)
        def _():
            make(c)

        @pl.when((c >= 1) & (c <= chunks))
        def _():
            pass_on(c - 1)

        @pl.when(c >= 3)
        def _():
            finish(c - 3)

        return 0

    down(0, 0, experts + 1, first=True)
    load_cw.wait()
    lax.fori_loop(0, chunks + 3, chunk, 0)
    for c in (chunks - 2, chunks - 1):
        result(c).wait()
        for i in range(4):
            pair(i, c).wait_send()
        for side in range(2):
            far(side, c).wait_send()
            near(side, c).wait_send()


def solution(mesh):
    n = mesh.shape["ep"]
    assert n == 8

    def body(x, expert, slot, gate, w_gate, w_up, w_down, s_gate, s_up, s_down):
        x, expert, slot, gate = x[0, 0], expert[0, 0], slot[0, 0], gate[0, 0]
        (tokens, depth), top = x.shape, expert.shape[1]
        experts, _, ff = w_gate.shape
        shared = s_gate.shape[1]
        slots = 5 * tokens * top // (4 * experts * n)
        pad = -(-slots // 16) * 16
        rows = experts * pad
        pieces, chunks, half = depth // PIECE, depth // OUT, tokens // 2
        top_k = 8
        assert top <= top_k and shared == 2 * ff and n * pad == tokens and rows % 128 == 0
        place = jnp.where(slot < slots, expert * pad + slot, -1).astype(F32)
        grow = ((0, 0), (0, top_k - top))
        info = jnp.concatenate([jnp.pad(place, grow, constant_values=-1), jnp.pad(gate, grow)], axis=1).T

        dma = pltpu.SemaphoreType.DMA
        h, cw, hs = pl.pallas_call(
            functools.partial(gather_kernel, n, slots),
            out_shape=(
                jax.ShapeDtypeStruct((experts, n * pad, ff), BF16),
                jax.ShapeDtypeStruct((n, tokens, rows), BF16),
                jax.ShapeDtypeStruct((2, tokens, ff), BF16),
            ),
            in_specs=[ANY] * 6,
            out_specs=(ANY,) * 3,
            scratch_shapes=[
                pltpu.VMEM((pieces, n, tokens, PIECE), BF16),
                pltpu.VMEM((n, 2 * top_k, tokens), F32),
                pltpu.VMEM((experts, n * pad, 2 * ff), F32),
                pltpu.VMEM((experts, n * pad, UNIT), BF16),
                pltpu.VMEM((n, rows, tokens), BF16),
                pltpu.VMEM((2, tokens, rows), BF16),
                pltpu.VMEM((2, n * pad, ff), BF16),
                pltpu.VMEM((RING, UNIT, 2 * ff), BF16),
                dma((pieces + 1,)),
                dma((n,)),
                dma((n,)),
                dma((8, pieces)),
                dma((8, pieces)),
                dma((RING, 2)),
                dma((2,)),
                dma((2,)),
            ],
            compiler_params=pltpu.CompilerParams(
                collective_id=0, has_side_effects=True, vmem_limit_bytes=VMEM_LIMIT
            ),
            name="gather",
        )(x, info, w_gate, w_up, s_gate, s_up)
        y = pl.pallas_call(
            functools.partial(reduce_kernel, n),
            out_shape=jax.ShapeDtypeStruct((tokens, depth), BF16),
            in_specs=[ANY] * 5,
            out_specs=ANY,
            scratch_shapes=[
                pltpu.VMEM((experts, n * pad, ff), BF16),
                pltpu.VMEM((n, tokens, rows), BF16),
                pltpu.VMEM((2, tokens, ff), BF16),
                pltpu.VMEM((2, SLAB // OUT, n, rows, OUT), BF16),
                pltpu.VMEM((2, SLAB // OUT, tokens, OUT), F32),
                pltpu.VMEM((2, 2, tokens, OUT), F32),
                pltpu.VMEM((4, tokens, OUT), F32),
                pltpu.VMEM((2, 4, tokens, OUT), BF16),
                pltpu.VMEM((2, tokens, OUT), BF16),
                pltpu.VMEM((2, 2, tokens, OUT), BF16),
                pltpu.VMEM((2, tokens, OUT), BF16),
                pltpu.VMEM((chunks, 4, tokens, OUT), BF16),
                pltpu.VMEM((chunks, 2, half, OUT), BF16),
                pltpu.VMEM((chunks, 2, tokens, OUT), BF16),
                pltpu.VMEM((DOWN_RING, ff, SLAB), BF16),
                pltpu.VMEM((2, shared, SLAB), BF16),
                dma((experts + 2,)),
                dma((4, 2)),
                dma((4, chunks)),
                dma((2, 2)),
                dma((2, chunks)),
                dma((2, 2)),
                dma((2, chunks)),
                dma((DOWN_RING,)),
                dma((2,)),
                dma((2,)),
            ],
            compiler_params=pltpu.CompilerParams(
                collective_id=1, has_side_effects=True, vmem_limit_bytes=VMEM_LIMIT
            ),
            name="reduce",
        )(h, cw, hs, w_down, s_down)
        return y[None, None]

    token, part, whole = P("dp", "ep"), P("ep"), P()
    return jax.shard_map(
        body,
        mesh=mesh,
        in_specs=(token,) * 4 + (part,) * 3 + (whole,) * 3,
        out_specs=token,
        check_vma=False,
    )
```

```python
import functools

import jax
import jax.numpy as jnp
from jax import lax
from jax.experimental import pallas as pl
from jax.experimental.pallas import tpu as pltpu
from jax.sharding import PartitionSpec as P

F32, BF16 = jnp.float32, jnp.bfloat16
MESH = pl.DeviceIdType.MESH
ANY = pl.BlockSpec(memory_space=pl.ANY)
VMEM_LIMIT = 67_043_328

PIECE = 256
UNIT = 512
OUT = 256
CUT = 512
AHEAD = 2
RING = 3
SPLIT = 5
SLAB = 512
DOWN_RING = 8

OWN, PARTNER, RIGHT, RIGHT_X, FAR, FAR_X, LEFT, LEFT_X = range(8)


def dot(a, b):
    return jnp.dot(a, b, preferred_element_type=F32)


def neighbours(n):
    me = lax.axis_index("ep")
    core = lax.rem(me, 2)
    chip = me // 2

    def at(slot):
        c = core if slot % 2 == 0 else 1 - core
        return 2 * lax.rem(chip + slot // 2, n // 2) + c

    return me, at


def greet(peers):
    barrier = pltpu.get_barrier_semaphore()
    for peer in peers:
        pl.semaphore_signal(barrier, inc=1, device_id={"ep": peer}, device_id_type=MESH)


def meet(peers):
    pl.semaphore_wait(pltpu.get_barrier_semaphore(), len(peers))


def gather_kernel(
    n, slots, x_hbm, info_hbm, wg_hbm, wu_hbm, sg_hbm, su_hbm,
    h_hbm, cw_hbm, hs_hbm,
    xg, info, acc, z, hot, cws, hstage, ring,
    load_sem, info_send, info_recv, send_sem, recv_sem, w_sem, cw_sem, h_sem,
):
    me, at = neighbours(n)
    tokens, depth = x_hbm.shape
    experts, _, ff = wg_hbm.shape
    pieces = depth // PIECE
    pad = z.shape[1] // n
    rows = experts * pad
    half = tokens // 2
    units, per = depth // UNIT, UNIT // PIECE
    shared_steps = 2 * units
    total = shared_steps + units * experts

    top, bottom, every = pl.ds(0, half), pl.ds(half, half), pl.ds(0, tokens)
    kinds = (
        (OWN, PARTNER, PARTNER, every),
        (OWN, LEFT, RIGHT, every),
        (OWN, RIGHT, LEFT, every),
        (LEFT, FAR, RIGHT, top),
        (RIGHT, FAR, LEFT, bottom),
        (LEFT, LEFT_X, PARTNER, every),
        (RIGHT, RIGHT_X, PARTNER, every),
        (FAR, FAR_X, PARTNER, every),
    )

    def move(kind, k):
        src, dst, to, r = kinds[kind]
        return pltpu.make_async_remote_copy(
            src_ref=xg.at[k, src, r, :],
            dst_ref=xg.at[k, dst, r, :],
            send_sem=send_sem.at[kind, k],
            recv_sem=recv_sem.at[kind, k],
            device_id={"ep": at(to)},
            device_id_type=MESH,
        )

    def opposite(slot):
        return 2 * ((n // 2 - slot // 2) % (n // 2)) + slot % 2

    def tell(slot):
        back = opposite(slot)
        return pltpu.make_async_remote_copy(
            src_ref=info.at[OWN],
            dst_ref=info.at[back],
            send_sem=info_send.at[slot],
            recv_sem=info_recv.at[back],
            device_id={"ep": at(slot)},
            device_id_type=MESH,
        )

    def load_x(k):
        return pltpu.make_async_copy(x_hbm.at[:, pl.ds(k * PIECE, PIECE)], xg.at[k, OWN], load_sem.at[k])

    load_info = pltpu.make_async_copy(info_hbm, info.at[OWN], load_sem.at[pieces])

    def fetch_shared(which, k, slot):
        w = (sg_hbm, su_hbm)[which]
        return pltpu.make_async_copy(w.at[pl.ds(k * UNIT, UNIT), :], ring.at[slot], w_sem.at[slot, 0])

    def fetch_routed(k, e, slot):
        return (
            pltpu.make_async_copy(wg_hbm.at[e, pl.ds(k * UNIT, UNIT), :], ring.at[slot, :, pl.ds(0, ff)], w_sem.at[slot, 0]),
            pltpu.make_async_copy(wu_hbm.at[e, pl.ds(k * UNIT, UNIT), :], ring.at[slot, :, pl.ds(ff, ff)], w_sem.at[slot, 1]),
        )

    def start(i):
        slot = lax.rem(i, RING)

        @pl.when(i < units)
        def _():
            fetch_shared(0, i, slot).start()

        @pl.when((i >= units) & (i < shared_steps))
        def _():
            fetch_shared(1, i - units, slot).start()

        @pl.when((i >= shared_steps) & (i < total))
        def _():
            j = i - shared_steps
            for c in fetch_routed(j // experts, lax.rem(j, experts), slot):
                c.start()

    def accumulate(a, left, slot, first):
        width = ring.shape[2]
        for lo in range(0, width, CUT):
            cut = pl.ds(lo, min(CUT, width - lo))
            before = jnp.where(first, 0.0, acc[a, :, cut])
            acc[a, :, cut] = before + dot(left, ring[slot, :, cut])

    everyone = [at(s) for s in range(1, n)]
    greet(everyone)
    for k in range(pieces):
        load_x(k).start()
    load_info.start()
    for i in range(RING - 1):
        fetch_shared(0, i, i).start()
    meet(everyone)
    for k in range(pieces):
        load_x(k).wait()
        if k < AHEAD:
            move(1, k).start()
            move(2, k).start()
        move(0, k).start()
        if k == 0:
            load_info.wait()
            for s in range(1, n):
                tell(s).start()

    def near(k):
        move(1, k).wait_recv()
        move(2, k).wait_recv()
        move(3, k).start()
        move(4, k).start()
        move(5, k).start()
        move(6, k).start()

        @pl.when(k + AHEAD < pieces)
        def _():
            move(1, k + AHEAD).start()
            move(2, k + AHEAD).start()

    def far(k):
        move(3, k).wait_recv()
        move(4, k).wait_recv()
        move(7, k).start()

    def shared_step(i, _):
        slot = lax.rem(i, RING)
        start(i + RING - 1)
        fetch_shared(0, 0, slot).wait()
        u = lax.rem(i, units)
        mine = jnp.concatenate([xg[u * per + p, OWN] for p in range(per)], axis=1)
        accumulate(i // units, mine, slot, u == 0)

        @pl.when(i == shared_steps - 3)
        def _():
            near(0)

        return 0

    lax.fori_loop(0, shared_steps, shared_step, 0)

    def hs_out(i):
        return pltpu.make_async_copy(hstage.at[i], hs_hbm.at[i], h_sem.at[i])

    for i in range(2):
        for lo in range(0, ff, 256):
            size = min(256, ff - lo)
            cut = pl.ds(i * ff + lo, size)
            hstage[i, :, pl.ds(lo, size)] = (jax.nn.silu(acc[0, :, cut]) * acc[1, :, cut]).astype(BF16)
        hs_out(i).start()

    top_k = info.shape[1] // 2
    first_row = (me * experts + lax.broadcasted_iota(jnp.int32, (experts, tokens), 0)) * pad
    first_row = first_row.astype(F32)
    in_slot = lax.broadcasted_iota(jnp.int32, (pad, tokens), 0).astype(F32)

    def table(s, weighted):
        at_slot = jnp.full((experts, tokens), -1.0, F32)
        weight = jnp.zeros((experts, tokens), F32)
        for j in range(top_k):
            here = info[s, pl.ds(j, 1), :] - first_row
            hit = (here >= 0) & (here < pad)
            at_slot = jnp.where(hit, here, at_slot)
            if weighted:
                weight = jnp.where(hit, info[s, pl.ds(top_k + j, 1), :], weight)
        return at_slot, weight

    for s in range(n):
        if s:
            tell(opposite(s)).wait_recv()
        at_slot, _ = table(s, False)
        for e in range(experts):
            hit = in_slot == at_slot[e : e + 1]
            hot[s, pl.ds(e * pad, pad), :] = jnp.where(hit, 1.0, 0.0).astype(BF16)

    near(1)

    def weigh(s):
        at_slot, weight = table(s, True)
        found = [jnp.where(in_slot == at_slot[e : e + 1], weight[e : e + 1], 0.0) for e in range(experts)]
        return jnp.concatenate(found, axis=0).T.astype(BF16)

    def cw_out(s):
        return pltpu.make_async_copy(cws.at[lax.rem(s, 2)], cw_hbm.at[s], cw_sem.at[lax.rem(s, 2)])

    def place(k, sources):
        for s in sources:
            whole = jnp.concatenate([xg[k + p, s] for p in range(per)], axis=1)
            got = dot(hot[s], whole).astype(BF16)
            for e in range(experts):
                z[e, s * pad : (s + 1) * pad, :] = got[e * pad : (e + 1) * pad]

    def place_near(k):
        for p in range(per):
            move(0, k + p).wait_recv()
            move(5, k + p).wait_recv()
            move(6, k + p).wait_recv()
        place(k, (OWN, PARTNER, RIGHT, LEFT, RIGHT_X, LEFT_X))

    def place_far(k):
        place(k, (FAR,))
        for p in range(per):
            move(7, k + p).wait_recv()
        place(k, (FAR_X,))

    def weigh_out(s):
        @pl.when(s >= 2)
        def _():
            cw_out(s - 2).wait()

        cws[lax.rem(s, 2)] = weigh(s)
        cw_out(s).start()

    assert per == 2

    def weigh_all(s, _):
        weigh_out(s)
        return 0

    lax.fori_loop(0, n, weigh_all, 0)
    far(0)
    place_near(0)
    near(2)
    far(1)
    place_far(0)

    def unit(u, _):
        def step(e, _):
            i = shared_steps + u * experts + e
            slot = lax.rem(i, RING)
            start(i + RING - 1)
            for c in fetch_routed(0, 0, slot):
                c.wait()
            accumulate(e, z[e], slot, u == 0)

            @pl.when((e == 1) | ((e == 6) & (2 * u + 4 < pieces)))
            def _():
                near(2 * u + 3 + e // 6)

            @pl.when(e == 4)
            def _():
                far(2 * u + 2)

            return 0

        lax.fori_loop(0, experts, step, 0)
        k = 2 * u + 2
        far(k + 1)
        place_near(k)
        place_far(k)
        return 0

    lax.fori_loop(0, units - 1, unit, 0)
    for i in range(2):
        hs_out(i).wait()
    last = units - 1

    def h_out(e):
        return pltpu.make_async_copy(hstage.at[lax.rem(e, 2)], h_hbm.at[e], h_sem.at[lax.rem(e, 2)])

    def final_step(e, _):
        i = shared_steps + last * experts + e
        slot = lax.rem(i, RING)
        start(i + RING - 1)
        for c in fetch_routed(0, 0, slot):
            c.wait()

        @pl.when(e >= 2)
        def _():
            h_out(e - 2).wait()

        for lo in range(0, ff, 256):
            size = min(256, ff - lo)
            a, b = pl.ds(lo, size), pl.ds(ff + lo, size)
            g = acc[e, :, a] + dot(z[e], ring[slot, :, a])
            u = acc[e, :, b] + dot(z[e], ring[slot, :, b])
            hstage[lax.rem(e, 2), :, a] = (jax.nn.silu(g) * u).astype(BF16)
        h_out(e).start()
        return 0

    lax.fori_loop(0, experts, final_step, 0)

    for s in (n - 2, n - 1):
        cw_out(s).wait()
    for e in (experts - 2, experts - 1):
        h_out(e).wait()
    for s in range(1, n):
        tell(s).wait_send()

    def drain(k, _):
        for kind in range(len(kinds)):
            move(kind, k).wait_send()
        return 0

    lax.fori_loop(0, pieces, drain, 0)


def reduce_kernel(
    n, h_hbm, cw_hbm, hs_hbm, wd_hbm, sd_hbm,
    y_hbm,
    h, cw, hs, out, yshared, ynear, yown, pair_out, far_out, near_out, ystage, pair_in, far_in, near_in, ring, sring,
    load_sem, pair_send, pair_recv, far_send, far_recv, near_send, near_recv, w_sem, s_sem, y_sem,
):
    me, at = neighbours(n)
    experts, rows_e, ff = h_hbm.shape
    tokens, depth = y_hbm.shape
    chunks = depth // OUT
    pad = rows_e // n
    half = tokens // 2
    per = SLAB // OUT
    assert per == 2 and DOWN_RING == experts
    slabs = chunks // per
    total = slabs * experts

    def columns(c):
        return pl.ds(pl.multiple_of(c * OUT, OUT), OUT)

    def load_h(e):
        return pltpu.make_async_copy(h_hbm.at[e], h.at[e], load_sem.at[e])

    load_cw = pltpu.make_async_copy(cw_hbm, cw, load_sem.at[experts])
    load_hs = pltpu.make_async_copy(hs_hbm, hs, load_sem.at[experts + 1])

    def slab(q):
        return pl.ds(pl.multiple_of(q * SLAB, SLAB), SLAB)

    def fetch(i):
        slot = lax.rem(i, DOWN_RING)
        return pltpu.make_async_copy(
            wd_hbm.at[lax.rem(i, experts), :, slab(i // experts)], ring.at[slot], w_sem.at[slot]
        )

    def fetch_shared(q):
        slot = lax.rem(q, 2)
        return pltpu.make_async_copy(sd_hbm.at[:, slab(q)], sring.at[slot], s_sem.at[slot])

    other = (FAR_X, RIGHT_X, LEFT_X, PARTNER)
    I_FAR, I_RIGHT, I_LEFT, I_OWN = range(4)

    def pair(i, c):
        return pltpu.make_async_remote_copy(
            src_ref=pair_out.at[lax.rem(c, 2), i],
            dst_ref=pair_in.at[c, i],
            send_sem=pair_send.at[i, lax.rem(c, 2)],
            recv_sem=pair_recv.at[i, c],
            device_id={"ep": at(PARTNER)},
            device_id_type=MESH,
        )

    def far(side, c):
        return pltpu.make_async_remote_copy(
            src_ref=far_out.at[lax.rem(c, 2), pl.ds(side * half, half), :],
            dst_ref=far_in.at[c, side],
            send_sem=far_send.at[side, lax.rem(c, 2)],
            recv_sem=far_recv.at[side, c],
            device_id={"ep": at((RIGHT, LEFT)[side])},
            device_id_type=MESH,
        )

    def near(side, c):
        return pltpu.make_async_remote_copy(
            src_ref=near_out.at[lax.rem(c, 2), side],
            dst_ref=near_in.at[c, side],
            send_sem=near_send.at[side, lax.rem(c, 2)],
            recv_sem=near_recv.at[side, c],
            device_id={"ep": at((RIGHT, LEFT)[side])},
            device_id_type=MESH,
        )

    def result(c):
        slot = lax.rem(c, 2)
        return pltpu.make_async_copy(ystage.at[slot], y_hbm.at[:, columns(c)], y_sem.at[slot])

    beside = [at(s) for s in (PARTNER, RIGHT, LEFT)]
    greet(beside)
    load_h(0).start()
    for i in range(experts):
        fetch(i).start()
        if i + 1 < experts:
            load_h(i + 1).start()
    load_cw.start()

    def down(q, begin, end, first=False):
        side = lax.rem(q, 2)

        def step(e, _):
            i = q * experts + e
            slot = lax.rem(i, DOWN_RING)
            fetch(i).wait()
            if first:
                load_h(e).wait()
            got = dot(h[e], ring[slot]).astype(BF16)
            at_row = pl.ds(pl.multiple_of(e * pad, pad), pad)
            for p in range(per):
                for s in range(n):
                    out[side, p, s, at_row, :] = got[s * pad : (s + 1) * pad, p * OUT : (p + 1) * OUT]

            @pl.when(i + DOWN_RING < total)
            def _():
                fetch(i + DOWN_RING).start()

            return 0

        lax.fori_loop(begin, min(end, experts), step, 0)
        if end > experts:
            fetch_shared(q).wait()
            got = dot(jnp.concatenate([hs[0], hs[1]], axis=1), sring[side])
            for p in range(per):
                yshared[side, p] = got[:, p * OUT : (p + 1) * OUT]

            @pl.when(q + 2 < slabs)
            def _():
                fetch_shared(q + 2).start()

    def make(c):
        side, p = lax.rem(c // per, 2), lax.rem(c, per)

        @pl.when(c >= 2)
        def _():
            for i in range(4):
                pair(i, c - 2).wait_send()
            for way in range(2):
                far(way, c - 2).wait_send()

        for i in range(4):
            s = other[i]
            pair_out[lax.rem(c, 2), i] = dot(cw[s], out[side, p, s]).astype(BF16)
            pair(i, c).start()
        ynear[lax.rem(c, 2), 0] = dot(cw[RIGHT], out[side, p, RIGHT])
        ynear[lax.rem(c, 2), 1] = dot(cw[LEFT], out[side, p, LEFT])
        own = dot(cw[OWN], out[side, p, OWN])
        mine = dot(cw[FAR], out[side, p, FAR])
        pair(I_FAR, c).wait_recv()
        far_out[lax.rem(c, 2)] = (mine + pair_in[c, I_FAR].astype(F32)).astype(BF16)
        far(0, c).start()
        far(1, c).start()

        @pl.when(c == 0)
        def _():
            load_hs.wait()
            down(0, experts, experts + 1)

        yown[lax.rem(c, 4)] = own + yshared[side, p]

    def ahead(c):
        for j in range(per):

            @pl.when((lax.rem(c, per) == j) & (c // per + 1 < slabs))
            def _():
                down(c // per + 1, (0, SPLIT)[j], (SPLIT, experts + 1)[j])

    def pass_on(c):
        slot = lax.rem(c, 2)

        @pl.when(c >= 2)
        def _():
            for side in range(2):
                near(side, c - 2).wait_send()

        for side, i in ((0, I_RIGHT), (1, I_LEFT)):
            pair(i, c).wait_recv()
            far(side, c).wait_recv()
            both, alone = pl.ds(side * half, half), pl.ds((1 - side) * half, half)
            near_out[slot, side, alone] = (ynear[slot, side, alone] + pair_in[c, i, alone].astype(F32)).astype(BF16)
            near_out[slot, side, both] = (
                ynear[slot, side, both] + pair_in[c, i, both].astype(F32) + far_in[c, side].astype(F32)
            ).astype(BF16)
            near(side, c).start()

    def finish(c):
        slot = lax.rem(c, 2)

        @pl.when(c >= 2)
        def _():
            result(c - 2).wait()

        pair(I_OWN, c).wait_recv()
        near(0, c).wait_recv()
        near(1, c).wait_recv()
        ystage[slot] = (
            yown[lax.rem(c, 4)]
            + pair_in[c, I_OWN].astype(F32)
            + near_in[c, 0].astype(F32)
            + near_in[c, 1].astype(F32)
        ).astype(BF16)
        result(c).start()

    def chunk(c, _):
        @pl.when(c < chunks)
        def _():
            make(c)

        @pl.when((c >= 1) & (c <= chunks))
        def _():
            pass_on(c - 1)

        @pl.when(c < chunks)
        def _():
            ahead(c)

        @pl.when(c >= 3)
        def _():
            finish(c - 3)

        return 0

    down(0, 0, experts, first=True)
    load_hs.start()
    fetch_shared(0).start()
    fetch_shared(1).start()
    load_cw.wait()
    meet(beside)
    lax.fori_loop(0, chunks + 3, chunk, 0)
    for c in (chunks - 2, chunks - 1):
        result(c).wait()
        for i in range(4):
            pair(i, c).wait_send()
        for side in range(2):
            far(side, c).wait_send()
            near(side, c).wait_send()


def solution(mesh):
    n = mesh.shape["ep"]
    assert n == 8

    def body(x, expert, slot, gate, w_gate, w_up, w_down, s_gate, s_up, s_down):
        x, expert, slot, gate = x[0, 0], expert[0, 0], slot[0, 0], gate[0, 0]
        (tokens, depth), top = x.shape, expert.shape[1]
        experts, _, ff = w_gate.shape
        shared = s_gate.shape[1]
        slots = 5 * tokens * top // (4 * experts * n)
        pad = -(-slots // 16) * 16
        rows = experts * pad
        pieces, chunks, half = depth // PIECE, depth // OUT, tokens // 2
        top_k = 8
        assert top <= top_k and shared == 2 * ff and n * pad == tokens and rows % 128 == 0
        place = jnp.where(slot < slots, expert * pad + slot, -1).astype(F32)
        grow = ((0, 0), (0, top_k - top))
        info = jnp.concatenate([jnp.pad(place, grow, constant_values=-1), jnp.pad(gate, grow)], axis=1).T

        dma = pltpu.SemaphoreType.DMA
        h, cw, hs = pl.pallas_call(
            functools.partial(gather_kernel, n, slots),
            out_shape=(
                jax.ShapeDtypeStruct((experts, n * pad, ff), BF16),
                jax.ShapeDtypeStruct((n, tokens, rows), BF16),
                jax.ShapeDtypeStruct((2, tokens, ff), BF16),
            ),
            in_specs=[ANY] * 6,
            out_specs=(ANY,) * 3,
            scratch_shapes=[
                pltpu.VMEM((pieces, n, tokens, PIECE), BF16),
                pltpu.VMEM((n, 2 * top_k, tokens), F32),
                pltpu.VMEM((experts, n * pad, 2 * ff), F32),
                pltpu.VMEM((experts, n * pad, UNIT), BF16),
                pltpu.VMEM((n, rows, tokens), BF16),
                pltpu.VMEM((2, tokens, rows), BF16),
                pltpu.VMEM((2, n * pad, ff), BF16),
                pltpu.VMEM((RING, UNIT, 2 * ff), BF16),
                dma((pieces + 1,)),
                dma((n,)),
                dma((n,)),
                dma((8, pieces)),
                dma((8, pieces)),
                dma((RING, 2)),
                dma((2,)),
                dma((2,)),
            ],
            compiler_params=pltpu.CompilerParams(
                collective_id=0, has_side_effects=True, vmem_limit_bytes=VMEM_LIMIT
            ),
            name="gather",
        )(x, info, w_gate, w_up, s_gate, s_up)
        y = pl.pallas_call(
            functools.partial(reduce_kernel, n),
            out_shape=jax.ShapeDtypeStruct((tokens, depth), BF16),
            in_specs=[ANY] * 5,
            out_specs=ANY,
            scratch_shapes=[
                pltpu.VMEM((experts, n * pad, ff), BF16),
                pltpu.VMEM((n, tokens, rows), BF16),
                pltpu.VMEM((2, tokens, ff), BF16),
                pltpu.VMEM((2, SLAB // OUT, n, rows, OUT), BF16),
                pltpu.VMEM((2, SLAB // OUT, tokens, OUT), F32),
                pltpu.VMEM((2, 2, tokens, OUT), F32),
                pltpu.VMEM((4, tokens, OUT), F32),
                pltpu.VMEM((2, 4, tokens, OUT), BF16),
                pltpu.VMEM((2, tokens, OUT), BF16),
                pltpu.VMEM((2, 2, tokens, OUT), BF16),
                pltpu.VMEM((2, tokens, OUT), BF16),
                pltpu.VMEM((chunks, 4, tokens, OUT), BF16),
                pltpu.VMEM((chunks, 2, half, OUT), BF16),
                pltpu.VMEM((chunks, 2, tokens, OUT), BF16),
                pltpu.VMEM((DOWN_RING, ff, SLAB), BF16),
                pltpu.VMEM((2, shared, SLAB), BF16),
                dma((experts + 2,)),
                dma((4, 2)),
                dma((4, chunks)),
                dma((2, 2)),
                dma((2, chunks)),
                dma((2, 2)),
                dma((2, chunks)),
                dma((DOWN_RING,)),
                dma((2,)),
                dma((2,)),
            ],
            compiler_params=pltpu.CompilerParams(
                collective_id=1, has_side_effects=True, vmem_limit_bytes=VMEM_LIMIT
            ),
            name="reduce",
        )(h, cw, hs, w_down, s_down)
        return y[None, None]

    token, part, whole = P("dp", "ep"), P("ep"), P()
    return jax.shard_map(
        body,
        mesh=mesh,
        in_specs=(token,) * 4 + (part,) * 3 + (whole,) * 3,
        out_specs=token,
        check_vma=False,
    )
```
